16 devices in a mesh: ep: 16 (over z, y, x, core).
Axes of the slice: x: 2, y: 2, z: 2, core: 2. Of those that a mesh axis runs over, the one named last changes fastest.
Arguments:
- x: bfloat16 [16384, 1024], P('ep')
- route_idx: int32 [16384, 8], P('ep')
- gates: bfloat16 [16384, 8], P('ep')
- dy: bfloat16 [16384, 1024], P('ep')
- w1: bfloat16 [32, 1024, 512], P('ep')
- w3: bfloat16 [32, 1024, 512], P('ep')
- w2: bfloat16 [32, 512, 1024], P('ep')
Outputs:
- output 1: bfloat16 [16384, 1024], P('ep')
- output 2: bfloat16 [16384, 1024], P('ep')
- output 3: float32 [32, 1024, 512], P('ep')
- output 4: float32 [32, 1024, 512], P('ep')
- output 5: float32 [32, 512, 1024], P('ep')
All inputs are finite; a program needn't handle non-finite values.
Results may differ from the reference program's by a relative error of at most 0.00103.
Values are sent between devices in bfloat16 or wider.
A program may use at most 1 GiB of HBM per device.

```python
import jax
import jax.numpy as jnp
from jax import lax

D = 1024
FF = 512
EXPERTS = 32
TOP = 8
TOKENS_DEV = 1024
EP = 16
HOT = 0
BLK = 64
TOKENS = TOKENS_DEV * EP
NONHOT = EXPERTS - 1


def setup_inputs(seed: int = 0) -> dict:
    ks = jax.random.split(jax.random.key(seed), 12)
    kd = jax.random.split(jax.random.fold_in(jax.random.key(seed), 7), 5)
    f32 = jnp.float32
    bf = jnp.bfloat16
    x = jax.random.normal(ks[0], (TOKENS, D), f32).astype(bf)
    dy = jax.random.normal(ks[1], (TOKENS, D), f32).astype(bf)
    w1 = (jax.random.normal(ks[2], (EXPERTS, D, FF), f32) * D ** -0.5).astype(bf)
    w3 = (jax.random.normal(ks[3], (EXPERTS, D, FF), f32) * D ** -0.5).astype(bf)
    w2 = (jax.random.normal(ks[4], (EXPERTS, FF, D), f32) * FF ** -0.5).astype(bf)
    src = jnp.arange(TOKENS) // TOKENS_DEV
    draw_r = jax.random.randint(kd[0], (EP,), 0, 1024, jnp.int32)
    prob_q = 102 + (901 * draw_r * draw_r) // (1024 * 1024)
    hot = jax.random.randint(kd[1], (TOKENS,), 0, 1024, jnp.int32) < prob_q[src]
    odd_idx = 2 * jnp.arange(TOKENS_DEV, dtype=jnp.int32) + 1
    levels = jnp.arange(1, NONHOT + 1, dtype=jnp.int32)
    below = 2 * TOKENS_DEV * levels[None, :] * levels[None, :] <= NONHOT * NONHOT * odd_idx[:, None]
    base = jnp.minimum(jnp.sum(below.astype(jnp.int32), axis=1), NONHOT - 1)
    shuf = jnp.argsort(jax.random.bits(kd[2], (EP, TOKENS_DEV), jnp.uint32), axis=1, stable=True)
    off = base[shuf].reshape(-1)
    relabel = jnp.argsort(jax.random.bits(kd[3], (EP, NONHOT), jnp.uint32), axis=1, stable=True)
    jj = jnp.arange(TOP)
    stride = NONHOT // TOP
    res = (off[:, None] + jj[None, :] * stride) % NONHOT
    cand = relabel[src[:, None], res]
    cand = cand + (cand >= HOT).astype(cand.dtype)
    pos = jax.random.randint(kd[4], (TOKENS,), 0, TOP)
    shift = hot[:, None] & (jj[None, :] > pos[:, None])
    route = jnp.take_along_axis(cand, jj[None, :] - shift.astype(jj.dtype), axis=1)
    is_h = hot[:, None] & (jj[None, :] == pos[:, None])
    route_idx = jnp.where(is_h, HOT, route).astype(jnp.int32)
    g = jax.random.uniform(ks[10], (TOKENS, TOP), f32, 0.2, 1.0)
    gh = jax.random.uniform(ks[11], (TOKENS, TOP), f32, 0.6, 1.0)
    gates = jnp.where(is_h, gh, g).astype(bf)
    return {'x': x, 'route_idx': route_idx, 'gates': gates, 'dy': dy, 'w1': w1, 'w3': w3, 'w2': w2}


def reference(x, route_idx, gates, dy, w1, w3, w2):
    f32 = jnp.float32
    bf = jnp.bfloat16
    ntok = x.shape[0]
    width = x.shape[1]
    nasg = ntok * TOP
    e_all = route_idx.reshape(-1)
    tok = jnp.arange(nasg) // TOP
    order = jnp.argsort(e_all, stable=True)
    e_sorted = e_all[order]
    counts = jnp.bincount(e_all, length=EXPERTS)
    padc = (counts + BLK - 1) // BLK * BLK
    pend = jnp.cumsum(padc)
    pstart = pend - padc
    gstart = jnp.cumsum(counts) - counts
    dest = pstart[e_sorted] + jnp.arange(nasg) - gstart[e_sorted]
    nrows = (nasg + BLK - 1) // BLK * BLK + EXPERTS * BLK
    nblk = nrows // BLK
    slot = jnp.full((nrows,), nasg, jnp.int32).at[dest].set(order.astype(jnp.int32))
    valid = slot < nasg
    sc = jnp.minimum(slot, nasg - 1)
    rows = jnp.where(valid, tok[sc], ntok)
    grow = jnp.where(valid, gates.reshape(-1)[sc].astype(f32), 0.0)
    xe = jnp.concatenate([x, jnp.zeros((1, width), x.dtype)], axis=0)
    dye = jnp.concatenate([dy, jnp.zeros((1, width), dy.dtype)], axis=0)
    starts = jnp.arange(nblk) * BLK
    bexp = jnp.minimum(jnp.sum((pend[None, :] <= starts[:, None]).astype(jnp.int32), axis=1), EXPERTS - 1)
    xb = xe[rows].reshape(nblk, BLK, width)
    dyb = dye[rows].reshape(nblk, BLK, width)
    gb = grow.reshape(nblk, BLK)

    def step(carry, inp):
        d1, d3, d2 = carry
        e, xr, gr, dyr = inp
        a1 = w1[e]
        a3 = w3[e]
        a2 = w2[e]
        u = jnp.dot(xr, a1, preferred_element_type=f32)
        v = jnp.dot(xr, a3, preferred_element_type=f32)
        sig = jax.nn.sigmoid(u)
        su = u * sig
        act = (su * v).astype(bf)
        o = jnp.dot(act, a2, preferred_element_type=f32).astype(bf)
        do = (gr[:, None] * dyr.astype(f32)).astype(bf)
        da = jnp.dot(do, a2.T, preferred_element_type=f32)
        du = (da * v * (sig * (1.0 + u * (1.0 - sig)))).astype(bf)
        dv = (da * su).astype(bf)
        dxk = (jnp.dot(du, a1.T, preferred_element_type=f32) + jnp.dot(dv, a3.T, preferred_element_type=f32)).astype(bf)
        d1 = d1.at[e].add(jnp.dot(xr.T, du, preferred_element_type=f32))
        d3 = d3.at[e].add(jnp.dot(xr.T, dv, preferred_element_type=f32))
        d2 = d2.at[e].add(jnp.dot(act.T, do, preferred_element_type=f32))
        return (d1, d3, d2), (o, dxk)

    init = (jnp.zeros(w1.shape, f32), jnp.zeros(w3.shape, f32), jnp.zeros(w2.shape, f32))
    (d1, d3, d2), (ob, dxb) = lax.scan(step, init, (bexp, xb, gb, dyb))
    contrib = ob.reshape(nrows, width).astype(f32) * grow[:, None]
    yf = jnp.zeros((ntok + 1, width), f32).at[rows].add(contrib)
    dxf = jnp.zeros((ntok + 1, width), f32).at[rows].add(dxb.reshape(nrows, width).astype(f32))
    return yf[:ntok].astype(bf), dxf[:ntok].astype(bf), d1, d3, d2
```

```python
import functools

import jax
import jax.numpy as jnp
from jax import lax
from jax.experimental import pallas as pl
from jax.experimental.pallas import tpu as pltpu
from jax.sharding import PartitionSpec as P

F32 = jnp.float32
BF = jnp.bfloat16
SUB = 256
CHUNKS = 4
NT = (((1,), (1,)), ((), ()))
TN = (((0,), (0,)), ((), ()))


def _dot(a, b):
    return jnp.dot(a, b, preferred_element_type=F32)


def _dot_nt(a, b):
    return lax.dot_general(a, b, NT, preferred_element_type=F32)


def _dot_tn(a, b):
    return lax.dot_general(a, b, TN, preferred_element_type=F32)


def _inner(x, dy, g, w1, w3, w2):
    on = g > 0.0
    u = _dot(x, w1)
    v = _dot(x, w3)
    sig = jax.nn.sigmoid(u)
    su = u * sig
    do = (g * dy.astype(F32)).astype(BF)
    da = _dot_nt(do, w2)
    act = jnp.where(on, su * v, 0.0).astype(BF)
    du = jnp.where(on, da * v * (sig * (1.0 + u * (1.0 - sig))), 0.0).astype(BF)
    dv = jnp.where(on, da * su, 0.0).astype(BF)
    return act, do, du, dv


def _home_kernel(slot, el, gd_ref, x_ref, dy_ref, w1_ref, w3_ref, w2_ref, yin_ref, dxin_ref, y_ref, dx_ref):
    s = pl.program_id(0)
    e = s * el + slot

    @pl.when(s == 0)
    def _():
        y_ref[...] = yin_ref[...]
        dx_ref[...] = dxin_ref[...]

    tl = x_ref.shape[0]
    w1 = w1_ref[0]
    w3 = w3_ref[0]
    w2 = w2_ref[0]

    @pl.loop(0, tl // SUB)
    def _(i):
        r = pl.ds(pl.multiple_of(i * SUB, SUB), SUB)
        gd = gd_ref[r, :]
        lane = lax.broadcasted_iota(jnp.int32, gd.shape, 1)
        g = jnp.sum(jnp.where(lane == e, gd, 0.0), axis=1, keepdims=True)
        act, _, du, dv = _inner(x_ref[r, :], dy_ref[r, :], g, w1, w3, w2)
        on = g > 0.0
        o = _dot(act, w2).astype(BF).astype(F32)
        y_ref[r, :] += jnp.where(on, g * o, 0.0)
        dxk = (_dot_nt(du, w1) + _dot_nt(dv, w3)).astype(BF).astype(F32)
        dx_ref[r, :] += jnp.where(on, dxk, 0.0)


def _home(slot, el, gd, x, dy, w1, w3, w2, y, dx):
    n, d, ff = w1.shape
    tl = x.shape[0]
    full = lambda a: pl.BlockSpec(a.shape, lambda s: (0,) * a.ndim, pipeline_mode=pl.Buffered(1))
    per = lambda a: pl.BlockSpec((1,) + a.shape[1:], lambda s: (s, 0, 0))
    return pl.pallas_call(
        functools.partial(_home_kernel, slot, el),
        grid=(n,),
        in_specs=[full(gd), full(x), full(dy), per(w1), per(w3), per(w2), full(y), full(dx)],
        out_specs=[full(y), full(dx)],
        out_shape=[jax.ShapeDtypeStruct(y.shape, F32)] * 2,
        input_output_aliases={6: 0, 7: 1},
        compiler_params=pltpu.CompilerParams(vmem_limit_bytes=60 << 20),
        cost_estimate=pl.CostEstimate(flops=n * tl * d * ff * 12, bytes_accessed=n * d * ff * 6, transcendentals=0),
        name='home',
    )(gd, x, dy, w1, w3, w2, y, dx)


def _owner_kernel(el, g_ref, x_ref, dy_ref, w1_ref, w3_ref, w2_ref, i1_ref, i3_ref, i2_ref, d1_ref, d3_ref, d2_ref):
    @pl.when(pl.program_id(0) == 0)
    def _():
        d1_ref[...] = i1_ref[...]
        d3_ref[...] = i3_ref[...]
        d2_ref[...] = i2_ref[...]

    x = x_ref[...]
    dy = dy_ref[...]
    gd = g_ref[...]

    @pl.loop(0, el)
    def _(e):
        lane = lax.broadcasted_iota(jnp.int32, gd.shape, 1)
        g = jnp.sum(jnp.where(lane == e, gd, 0.0), axis=1, keepdims=True)
        act, do, du, dv = _inner(x, dy, g, w1_ref[e], w3_ref[e], w2_ref[e])
        d1_ref[e] += _dot_tn(x, du)
        d3_ref[e] += _dot_tn(x, dv)
        d2_ref[e] += _dot_tn(act, do)


def _owner(gt, x, dy, w1, w3, w2, a1, a3, a2, block):
    el, d, ff = w1.shape
    rows = x.shape[0]
    full = lambda a: pl.BlockSpec(a.shape, lambda s: (0,) * a.ndim, pipeline_mode=pl.Buffered(1))
    per = lambda a: pl.BlockSpec((block, a.shape[1]), lambda s: (s, 0))
    return pl.pallas_call(
        functools.partial(_owner_kernel, el),
        grid=(rows // block,),
        in_specs=[per(gt), per(x), per(dy)] + [full(a) for a in (w1, w3, w2, a1, a3, a2)],
        out_specs=[full(a) for a in (a1, a3, a2)],
        out_shape=[jax.ShapeDtypeStruct(a.shape, F32) for a in (a1, a3, a2)],
        input_output_aliases={6: 0, 7: 1, 8: 2},
        compiler_params=pltpu.CompilerParams(vmem_limit_bytes=60 << 20),
        cost_estimate=pl.CostEstimate(flops=rows * el * d * ff * 12, bytes_accessed=rows * d * 4, transcendentals=0),
        name='owner',
    )(gt, x, dy, w1, w3, w2, a1, a3, a2)


def solution(mesh):
    n = mesh.shape['ep']

    def body(xl, rl, gl, dyl, w1l, w3l, w2l):
        tl, d = xl.shape
        el, _, ff = w1l.shape
        nexp = el * n
        gather = lambda a: lax.all_gather(a, 'ep', axis=0, tiled=True)
        hit = rl[:, :, None] == jnp.arange(nexp)[None, None, :]
        gd = jnp.sum(jnp.where(hit, gl.astype(F32)[:, :, None], 0.0), axis=1)
        mine = lax.all_to_all(gd.reshape(tl, n, el).transpose(1, 0, 2), 'ep', 0, 0, tiled=True)

        ws = [[gather(a[s:s + 1]) for a in (w1l, w3l, w2l)] for s in range(el)]
        ws[0][0], xg, dyg = lax.optimization_barrier((ws[0][0], xl, dyl))
        y = jnp.zeros((tl, d), F32)
        dx = jnp.zeros((tl, d), F32)
        for s in range(el):
            y, dx = _home(s, el, gd, xl, dyl, *ws[s], y, dx)

        step = tl // CHUNKS
        acc = (jnp.zeros((el, d, ff), F32), jnp.zeros((el, d, ff), F32), jnp.zeros((el, ff, d), F32))
        for c in range(CHUNKS):
            r = slice(c * step, (c + 1) * step)
            gt = mine[:, r].reshape(n * step, el)
            acc = _owner(gt, gather(xg[r]), gather(dyg[r]), w1l, w3l, w2l, *acc, 512)
        return (y.astype(BF), dx.astype(BF)) + tuple(acc)

    spec_t = P('ep', None)
    spec_w = P('ep', None, None)
    return jax.shard_map(body, mesh=mesh, in_specs=(spec_t, spec_t, spec_t, spec_t, spec_w, spec_w, spec_w), out_specs=(spec_t, spec_t, spec_w, spec_w, spec_w), check_vma=False)
```

```python
import functools

import jax
import jax.numpy as jnp
from jax import lax
from jax.experimental import pallas as pl
from jax.experimental.pallas import tpu as pltpu
from jax.sharding import PartitionSpec as P

F32 = jnp.float32
BF = jnp.bfloat16
MESH = pl.DeviceIdType.MESH
NT = (((1,), (1,)), ((), ()))
TN = (((0,), (0,)), ((), ()))
BITS = (2, 4, 8)

ROUNDS = (
    lambda l: (l, ()),
    lambda l: ((l + 2) % 3, ()),
    lambda l: ((l + 1) % 3, ()),
    lambda l: ((l + 2) % 3, ((l + 2) % 3,)),
    lambda l: ((l + 1) % 3, ((l + 1) % 3,)),
    lambda l: ((l + 1) % 3, ((l + 2) % 3,)),
    lambda l: ((l + 1) % 3, ((l + 1) % 3, (l + 2) % 3)),
)
WROUNDS = ([(0, r) for r in range(3)] + [(1, r) for r in range(3)] + [(0, r) for r in range(3, 6)]
           + [(1, r) for r in range(3, 6)] + [(0, 6), (1, 6)])
SERVICE = {
    ('t', 0): (3, [('t', 3), ('t', 4)]),
    ('t', 1): (6, [('t', 5)]),
    ('t', 2): (6, []),
    ('t', 3): (9, [('t', 6), ('w', 0)]),
    ('t', 4): (11, [('w', 1)]),
    ('t', 5): (12, [('w', 2)]),
    ('t', 6): (15, [('w', 3)]),
    ('w', 0): (16, [('w', 4)]),
    ('w', 1): (18, [('w', 5)]),
    ('w', 2): (19, [('w', 6)]),
    ('w', 3): (22, [('w', 7)]),
    ('w', 4): (24, [('w', 8)]),
    ('w', 5): (26, [('w', 9)]),
    ('w', 6): (30, [('w', 10)]),
    ('w', 7): (32, [('w', 11)]),
    ('w', 8): (32, [('w', 12)]),
    ('w', 9): (36, [('w', 13)]),
    ('w', 10): (38, []),
    ('w', 11): (38, []),
    ('w', 12): (42, []),
    ('w', 13): (45, []),
}
PASSED = {8: [('t', r) for r in range(3)], 14: [('t', r) for r in range(3, 6)], 18: [('t', 6)],
          22: [('w', r) for r in range(3)], 28: [('w', r) for r in range(3, 6)], 34: [('w', r) for r in range(6, 9)],
          40: [('w', r) for r in range(9, 12)], 44: [('w', 12)], 46: [('w', 13)]}
TSTART = (0, 1, 2, 8)
WSTART = (0, 4, 10, 16, 22)
STEPS = 48


def _dot(a, b):
    return jnp.dot(a, b, preferred_element_type=F32)


def _dot_nt(a, b):
    return lax.dot_general(a, b, NT, preferred_element_type=F32)


def _dot_tn(a, b):
    return lax.dot_general(a, b, TN, preferred_element_type=F32)


def _column(gd, e):
    lane = lax.broadcasted_iota(jnp.int32, gd.shape, 1)
    return jnp.sum(jnp.where(lane == e, gd, 0.0), axis=1, keepdims=True)


def _inner(x, dy, g, w1, w3, w2):
    on = g > 0.0
    u = _dot(x, w1)
    v = _dot(x, w3)
    sig = jax.nn.sigmoid(u)
    su = u * sig
    do = (g * dy.astype(F32)).astype(BF)
    da = _dot_nt(do, w2)
    act = jnp.where(on, su * v, 0.0).astype(BF)
    du = jnp.where(on, da * v * (sig * (1.0 + u * (1.0 - sig))), 0.0).astype(BF)
    dv = jnp.where(on, da * su, 0.0).astype(BF)
    return act, do, du, dv


def _flip(dev, bit):
    return dev + bit * (1 - 2 * ((dev // bit) % 2))


def _cross(dev, links):
    for l in links:
        dev = _flip(dev, BITS[l])
    return dev


def _source(me, j, c):
    m = j + jnp.where(j == 3, 1, 0) - jnp.where(j == 4, 1, 0)
    dev = me
    for i, on in enumerate((c, m % 2, (m // 2) % 2, m // 4)):
        bit = 2 ** i
        dev = dev + on * bit * (1 - 2 * ((me // bit) % 2))
    return dev


def _group(q, base):
    return base + q % 3, q // 3


def _kernel(el, thirds, x_ref, dy_ref, w1_ref, w3_ref, w2_ref, gd_ref, gm_ref,
            y_ref, dx_ref, d1_ref, d3_ref, d2_ref, xa, dya, wa1, wa3, wa2,
            tx, tdy, tg, v1, v3, v2, o1, o3, o2, ox, ody, og, yacc, dxacc, a1, a3, a2,
            ts, tr, ws, wr, tps, tpr, wps, wpr, tos, tor, wos, wor, tl_sem, wl_sem, own_sem, out_sem):
    me = lax.axis_index('ep')
    other = _flip(me, 1)
    near = [_flip(me, b) for b in BITS]

    def remote(src, dst, ssem, rsem, dev):
        return pltpu.make_async_remote_copy(src_ref=src, dst_ref=dst, send_sem=ssem, recv_sem=rsem,
                                            device_id=(dev,), device_id_type=MESH)

    def pieces(kind, r, p, dev, mine, k):
        if kind == 't':
            rows = pl.ds(*thirds[p])
            return [((x_ref if mine else xa.at[dev]).at[rows], xa.at[dev, rows], (r, k, 0)),
                    ((dy_ref if mine else dya.at[dev]).at[rows], dya.at[dev, rows], (r, k, 1))]
        slot = WROUNDS[r][0]
        own, far = ((w1_ref, wa1), (w3_ref, wa3), (w2_ref, wa2))[p]
        return [(own.at[slot] if mine else far.at[dev * el + slot], far.at[dev * el + slot], (r, k))]

    def item_round(kind, r):
        return r if kind == 't' else WROUNDS[r][1]

    def sent(kind, r):
        ss, rs = (ts, tr) if kind == 't' else (ws, wr)
        out = []
        for l in range(3):
            p, path = ROUNDS[item_round(kind, r)](l)
            for src, dst, i in pieces(kind, r, p, _cross(me, path), not path, l):
                out.append(remote(src, dst, ss.at[i], rs.at[i], near[l]))
        return out

    def arrived(kind, r, at, ss, rs, dev):
        out = []
        for l in range(3):
            p, path = ROUNDS[item_round(kind, r)](l)
            for _, dst, i in pieces(kind, r, p, _cross(at, path + (l,)), False, l):
                out.append(remote(dst, dst, ss.at[i], rs.at[i], near[l] if dev is None else dev))
        return out

    def received(kind, r):
        return arrived(kind, r, me, *((ts, tr) if kind == 't' else (ws, wr)), None)

    def passed(kind, r):
        return arrived(kind, r, me, *((tps, tpr) if kind == 't' else (wps, wpr)), other)

    def passed_here(kind, r):
        return arrived(kind, r, other, *((tps, tpr) if kind == 't' else (wps, wpr)), other)

    def own_pass_t(dev):
        return [remote(x_ref, xa.at[dev], tos.at[0], tor.at[0], other),
                remote(dy_ref, dya.at[dev], tos.at[1], tor.at[1], other)]

    def own_pass_w(dev):
        return [remote(own.at[s], far.at[dev * el + s], wos.at[s, i], wor.at[s, i], other)
                for s in range(el) for i, (own, far) in enumerate(((w1_ref, wa1), (w3_ref, wa3), (w2_ref, wa2)))]

    def start(copies):
        for c in copies:
            c.start()

    own_loads = [pltpu.make_async_copy(a, b, own_sem.at[i]) for i, (a, b) in enumerate((
        (x_ref, ox), (dy_ref, ody), (gd_ref, og), (w1_ref, o1), (w3_ref, o3), (w2_ref, o2)))]
    start(own_loads)

    barrier = pltpu.get_barrier_semaphore()
    for dev in near + [other]:
        pl.semaphore_signal(barrier, inc=1, device_id=(dev,), device_id_type=MESH)
    pl.semaphore_wait(barrier, 4)
    for r in range(3):
        start(sent('t', r))
    start(own_pass_t(me))
    start(own_pass_w(me))

    yacc[...] = jnp.zeros_like(yacc)
    dxacc[...] = jnp.zeros_like(dxacc)
    a1[...] = jnp.zeros_like(a1)
    a3[...] = jnp.zeros_like(a3)
    a2[...] = jnp.zeros_like(a2)
    for c in own_loads:
        c.wait()

    def t_source(k):
        near_j, near_c = _group(k - 2, 1)
        mid_j, mid_c = _group(k - 8, 4)
        j = jnp.where(k < 2, 0, jnp.where(k < 8, near_j, jnp.where(k < 14, mid_j, 7)))
        c = jnp.where(k < 2, k, jnp.where(k < 8, near_c, jnp.where(k < 14, mid_c, k - 14)))
        return _source(me, j, c)

    def w_source(k):
        q = k - 4
        g = q // 6
        gj, gc = _group(q % 6, jnp.where(g < 2, 1, 4))
        j = jnp.where(k < 4, 0, jnp.where(k < 28, gj, 7))
        c = jnp.where(k < 4, k // 2, jnp.where(k < 28, gc, k % 2))
        slot = jnp.where(k < 4, k % 2, jnp.where(k < 28, g % 2, (k - 28) // 2))
        return _source(me, j, c) * el + slot

    def t_load(k, own):
        b = k % 2
        dev = t_source(k)
        return [pltpu.make_async_copy(x_ref if own else xa.at[dev], tx.at[b], tl_sem.at[b, 0]),
                pltpu.make_async_copy(dy_ref if own else dya.at[dev], tdy.at[b], tl_sem.at[b, 1]),
                pltpu.make_async_copy(gm_ref.at[dev], tg.at[b], tl_sem.at[b, 2])]

    def w_load(k, own):
        b = k % 2
        e = w_source(k)
        s = k % 2
        return [pltpu.make_async_copy(w1_ref.at[s] if own else wa1.at[e], v1.at[b], wl_sem.at[b, 0]),
                pltpu.make_async_copy(w3_ref.at[s] if own else wa3.at[e], v3.at[b], wl_sem.at[b, 1]),
                pltpu.make_async_copy(w2_ref.at[s] if own else wa2.at[e], v2.at[b], wl_sem.at[b, 2])]

    def fetch(load, k, owned):
        @pl.when(k < owned)
        def _():
            start(load(k, True))

        @pl.when(k >= owned)
        def _():
            start(load(k, False))

    def any_of(k, values):
        hit = k == values[0]
        for v in values[1:]:
            hit = jnp.logical_or(hit, k == v)
        return hit

    def turn(load, k, owned, starts, count):
        @pl.when(any_of(k, starts))
        def _():
            fetch(load, k, owned)

        @pl.when(jnp.logical_and(k + 1 < count, jnp.logical_not(any_of(k + 1, starts))))
        def _():
            fetch(load, k + 1, owned)

        for c in load(k, False):
            c.wait()

    @pl.loop(0, STEPS)
    def _(s):
        for key, (at, sends) in SERVICE.items():
            @pl.when(s == at)
            def _(key=key, sends=sends):
                for c in received(*key):
                    c.wait_recv()
                start(passed(*key))
                for k in sends:
                    start(sent(*k))

        @pl.when(s == 1)
        def _():
            for c in own_pass_t(other):
                c.wait_recv()

        @pl.when(s == 3)
        def _():
            for c in own_pass_w(other):
                c.wait_recv()

        for at, keys in PASSED.items():
            @pl.when(s == at)
            def _(keys=keys):
                for key in keys:
                    for c in passed_here(*key):
                        c.wait_recv()

        tokens = jnp.logical_or(s < 2, jnp.logical_and(s >= 6, s < 20))

        @pl.when(tokens)
        def _():
            k = jnp.where(s < 2, s, s - 4)
            b = k % 2
            turn(t_load, k, 1, TSTART, 16)

            @pl.loop(0, el)
            def _(e):
                x = tx[b]
                act, do, du, dv = _inner(x, tdy[b], _column(tg[b], e), o1[e], o3[e], o2[e])
                a1[e] += _dot_tn(x, du)
                a3[e] += _dot_tn(x, dv)
                a2[e] += _dot_tn(act, do)

        @pl.when(jnp.logical_not(tokens))
        def _():
            k = jnp.where(s < 6, s - 2, s - 16)
            b = k % 2
            turn(w_load, k, 2, WSTART, 32)
            g = _column(og[...], w_source(k))
            act, _, du, dv = _inner(ox[...], ody[...], g, v1[b], v3[b], v2[b])
            on = g > 0.0
            o = _dot(act, v2[b]).astype(BF).astype(F32)
            yacc[...] += jnp.where(on, g * o, 0.0)
            dxk = (_dot_nt(du, v1[b]) + _dot_nt(dv, v3[b])).astype(BF).astype(F32)
            dxacc[...] += jnp.where(on, dxk, 0.0)

        @pl.when(s == 20)
        def _():
            for i, (a, d) in enumerate(((a1, d1_ref), (a3, d3_ref), (a2, d2_ref))):
                pltpu.make_async_copy(a, d, out_sem.at[i]).start()

    tx[0] = yacc[...].astype(BF)
    tx[1] = dxacc[...].astype(BF)
    outs = [pltpu.make_async_copy(tx.at[0], y_ref, out_sem.at[3]), pltpu.make_async_copy(tx.at[1], dx_ref, out_sem.at[4])]
    start(outs)
    for i, (a, d) in enumerate(((a1, d1_ref), (a3, d3_ref), (a2, d2_ref))):
        pltpu.make_async_copy(a, d, out_sem.at[i]).wait()
    for key in SERVICE:
        for c in sent(*key) + passed(*key):
            c.wait_send()
    for c in own_pass_t(me) + own_pass_w(me):
        c.wait_send()
    for c in outs:
        c.wait()


def solution(mesh):
    n = mesh.shape['ep']

    def body(xl, rl, gl, dyl, w1l, w3l, w2l):
        tl, d = xl.shape
        el, _, ff = w1l.shape
        nexp = el * n
        hit = rl[:, :, None] == jnp.arange(nexp)[None, None, :]
        gd = jnp.sum(jnp.where(hit, gl.astype(F32)[:, :, None], 0.0), axis=1)
        gm = lax.all_to_all(gd.reshape(tl, n, el).transpose(1, 0, 2), 'ep', 0, 0, tiled=True)

        third = -(-tl // 48) * 16
        thirds = ((0, third), (third, (tl - third) // 2), ((tl + third) // 2, (tl - third) // 2))
        dma = pltpu.SemaphoreType.DMA
        out = lambda *s: jax.ShapeDtypeStruct(s, F32)
        outb = lambda *s: jax.ShapeDtypeStruct(s, BF)
        nw = len(WROUNDS)
        hbm = pl.BlockSpec(memory_space=pl.ANY)
        res = pl.pallas_call(
            functools.partial(_kernel, el, thirds),
            out_shape=[outb(tl, d), outb(tl, d), out(el, d, ff), out(el, d, ff), out(el, ff, d),
                       outb(n, tl, d), outb(n, tl, d), outb(nexp, d, ff), outb(nexp, d, ff), outb(nexp, ff, d)],
            in_specs=[hbm] * 7,
            out_specs=[hbm] * 10,
            scratch_shapes=[
                pltpu.VMEM((2, tl, d), BF), pltpu.VMEM((2, tl, d), BF), pltpu.VMEM((2, tl, el), F32),
                pltpu.VMEM((2, d, ff), BF), pltpu.VMEM((2, d, ff), BF), pltpu.VMEM((2, ff, d), BF),
                pltpu.VMEM((el, d, ff), BF), pltpu.VMEM((el, d, ff), BF), pltpu.VMEM((el, ff, d), BF),
                pltpu.VMEM((tl, d), BF), pltpu.VMEM((tl, d), BF), pltpu.VMEM((tl, nexp), F32),
                pltpu.VMEM((tl, d), F32), pltpu.VMEM((tl, d), F32),
                pltpu.VMEM((el, d, ff), F32), pltpu.VMEM((el, d, ff), F32), pltpu.VMEM((el, ff, d), F32),
                dma((7, 3, 2)), dma((7, 3, 2)), dma((nw, 3)), dma((nw, 3)),
                dma((7, 3, 2)), dma((7, 3, 2)), dma((nw, 3)), dma((nw, 3)),
                dma((2,)), dma((2,)), dma((el, 3)), dma((el, 3)),
                dma((2, 3)), dma((2, 3)), dma((6,)), dma((5,)),
            ],
            compiler_params=pltpu.CompilerParams(collective_id=0, has_side_effects=True, vmem_limit_bytes=67043328),
            name='moe',
        )(xl, dyl, w1l, w3l, w2l, gd, gm)
        return tuple(res[:5])

    spec_t = P('ep', None)
    spec_w = P('ep', None, None)
    return jax.shard_map(body, mesh=mesh, in_specs=(spec_t, spec_t, spec_t, spec_t, spec_w, spec_w, spec_w), out_specs=(spec_t, spec_t, spec_w, spec_w, spec_w), check_vma=False)
```

```python
import functools

import jax
import jax.numpy as jnp
from jax import lax
from jax.experimental import pallas as pl
from jax.experimental.pallas import tpu as pltpu
from jax.sharding import PartitionSpec as P

F32 = jnp.float32
BF = jnp.bfloat16
MESH = pl.DeviceIdType.MESH
NT = (((1,), (1,)), ((), ()))
TN = (((0,), (0,)), ((), ()))
BITS = (2, 4, 8)

ROUNDS = (
    lambda l: (l, ()),
    lambda l: ((l + 2) % 3, ()),
    lambda l: ((l + 1) % 3, ()),
    lambda l: ((l + 2) % 3, ((l + 2) % 3,)),
    lambda l: ((l + 1) % 3, ((l + 1) % 3,)),
    lambda l: ((l + 1) % 3, ((l + 2) % 3,)),
    lambda l: ((l + 1) % 3, ((l + 1) % 3, (l + 2) % 3)),
)
SPREAD = ((4, 3, 5), (3, 5, 4), (4, 3, 5))
WROUNDS = ([(0, r) for r in range(3)] + [(1, r) for r in range(3)] + [(0, r) for r in range(3, 6)]
           + [(1, r) for r in range(3, 6)] + [(0, 6), (1, 6)])
SERVICE = {
    ('t', 0): (3, [('t', 3), ('t', 4)]),
    ('t', 1): (6, [('t', 5)]),
    ('t', 2): (6, []),
    ('t', 3): (9, [('t', 6), ('w', 0)]),
    ('t', 4): (11, [('w', 1)]),
    ('t', 5): (12, [('w', 2)]),
    ('t', 6): (15, [('w', 3)]),
    ('w', 0): (16, [('w', 4)]),
    ('w', 1): (18, [('w', 5)]),
    ('w', 2): (19, [('w', 6)]),
    ('w', 3): (22, [('w', 7)]),
    ('w', 4): (24, [('w', 8)]),
    ('w', 5): (26, [('w', 9)]),
    ('w', 6): (30, [('w', 10)]),
    ('w', 7): (32, [('w', 11)]),
    ('w', 8): (34, [('w', 12)]),
    ('w', 9): (38, []),
    ('w', 10): (38, [('w', 13)]),
    ('w', 11): (40, []),
    ('w', 12): (44, []),
    ('w', 13): (46, []),
}
PASSED = {8: [('t', r) for r in range(3)], 14: [('t', r) for r in range(3, 6)], 18: [('t', 6)],
          22: [('w', r) for r in range(3)], 28: [('w', r) for r in range(3, 6)], 33: [('w', 6), ('w', 7)], 35: [('w', 8)],
          39: [('w', 9), ('w', 10)], 41: [('w', 11)], 45: [('w', 12)], 47: [('w', 13)]}
TSTART = (0, 1, 2, 8)
WSTART = (0, 4, 10, 16, 17, 18, 22, 23, 24, 28, 29, 30, 31)
STEPS = 48


def _dot(a, b):
    return jnp.dot(a, b, preferred_element_type=F32)


def _dot_nt(a, b):
    return lax.dot_general(a, b, NT, preferred_element_type=F32)


def _dot_tn(a, b):
    return lax.dot_general(a, b, TN, preferred_element_type=F32)


def _column(gd, e):
    lane = lax.broadcasted_iota(jnp.int32, gd.shape, 1)
    return jnp.sum(jnp.where(lane == e, gd, 0.0), axis=1, keepdims=True)


def _inner(x, dy, g, w1, w3, w2):
    on = g > 0.0
    u = _dot(x, w1)
    v = _dot(x, w3)
    sig = jax.nn.sigmoid(u)
    su = u * sig
    do = (g * dy.astype(F32)).astype(BF)
    da = _dot_nt(do, w2)
    act = jnp.where(on, su * v, 0.0).astype(BF)
    du = jnp.where(on, da * v * (sig * (1.0 + u * (1.0 - sig))), 0.0).astype(BF)
    dv = jnp.where(on, da * su, 0.0).astype(BF)
    return act, do, du, dv


def _flip(dev, bit):
    return dev + bit * (1 - 2 * ((dev // bit) % 2))


def _cross(dev, links):
    for l in links:
        dev = _flip(dev, BITS[l])
    return dev


def _source(me, j, c):
    m = j + jnp.where(j == 3, 1, 0) - jnp.where(j == 4, 1, 0)
    dev = me
    for i, on in enumerate((c, m % 2, (m // 2) % 2, m // 4)):
        bit = 2 ** i
        dev = dev + on * bit * (1 - 2 * ((me // bit) % 2))
    return dev


def _group(q, base):
    return base + q % 3, q // 3


def _kernel(el, thirds, x_ref, dy_ref, gt_ref, w1_ref, w3_ref, w2_ref,
            y_ref, dx_ref, d1_ref, d3_ref, d2_ref, xa, dya, gta, wa1, wa3, wa2,
            tx, tdy, tg, v1, v3, v2, o1, o3, o2, ox, ody, og, yacc, dxacc, a1, a3, a2,
            ts, tr, ws, wr, tps, tpr, wps, wpr, tos, tor, wos, wor, tl_sem, wl_sem, own_sem, out_sem):
    me = lax.axis_index('ep')
    other = _flip(me, 1)
    near = [_flip(me, b) for b in BITS]

    def remote(src, dst, ssem, rsem, dev):
        return pltpu.make_async_remote_copy(src_ref=src, dst_ref=dst, send_sem=ssem, recv_sem=rsem,
                                            device_id=(dev,), device_id_type=MESH)

    def pieces(kind, r, p, dev, mine, k):
        if kind == 't':
            rows = pl.ds(*thirds[p])
            gate = [(gt_ref if mine else gta.at[dev], gta.at[dev], (r, k, 2))] if p == 0 else []
            return gate + [((x_ref if mine else xa.at[dev]).at[rows], xa.at[dev, rows], (r, k, 0)),
                           ((dy_ref if mine else dya.at[dev]).at[rows], dya.at[dev, rows], (r, k, 1))]
        slot = WROUNDS[r][0]
        own, far = ((w1_ref, wa1), (w3_ref, wa3), (w2_ref, wa2))[p]
        return [(own.at[slot] if mine else far.at[dev * el + slot], far.at[dev * el + slot], (r, k))]

    def leg(kind, r, l):
        i = r if kind == 't' else WROUNDS[r][1]
        if kind == 'w' and 3 <= i < 6:
            i = SPREAD[l][i - 3]
        return ROUNDS[i](l)

    def sent(kind, r):
        ss, rs = (ts, tr) if kind == 't' else (ws, wr)
        out = []
        for l in range(3):
            p, path = leg(kind, r, l)
            for src, dst, i in pieces(kind, r, p, _cross(me, path), not path, l):
                out.append(remote(src, dst, ss.at[i], rs.at[i], near[l]))
        return out

    def arrived(kind, r, at, ss, rs, dev):
        out = []
        for l in range(3):
            p, path = leg(kind, r, l)
            for _, dst, i in pieces(kind, r, p, _cross(at, path + (l,)), False, l):
                out.append(remote(dst, dst, ss.at[i], rs.at[i], near[l] if dev is None else dev))
        return out

    def received(kind, r):
        return arrived(kind, r, me, *((ts, tr) if kind == 't' else (ws, wr)), None)

    def passed(kind, r):
        return arrived(kind, r, me, *((tps, tpr) if kind == 't' else (wps, wpr)), other)

    def passed_here(kind, r):
        return arrived(kind, r, other, *((tps, tpr) if kind == 't' else (wps, wpr)), other)

    def own_pass_t(dev):
        return [remote(x_ref, xa.at[dev], tos.at[0], tor.at[0], other),
                remote(dy_ref, dya.at[dev], tos.at[1], tor.at[1], other),
                remote(gt_ref, gta.at[dev], tos.at[2], tor.at[2], other)]

    def own_pass_w(dev):
        return [remote(own.at[s], far.at[dev * el + s], wos.at[s, i], wor.at[s, i], other)
                for s in range(el) for i, (own, far) in enumerate(((w1_ref, wa1), (w3_ref, wa3), (w2_ref, wa2)))]

    def start(copies):
        for c in copies:
            c.start()

    own_loads = [pltpu.make_async_copy(a, b, own_sem.at[i]) for i, (a, b) in enumerate((
        (x_ref, ox), (dy_ref, ody), (gt_ref, tg.at[1]), (w1_ref, o1), (w3_ref, o3), (w2_ref, o2)))]
    start(own_loads)

    barrier = pltpu.get_barrier_semaphore()
    for dev in near + [other]:
        pl.semaphore_signal(barrier, inc=1, device_id=(dev,), device_id_type=MESH)
    pl.semaphore_wait(barrier, 4)
    for r in range(3):
        start(sent('t', r))
    start(own_pass_t(me))
    start(own_pass_w(me))

    yacc[...] = jnp.zeros_like(yacc)
    dxacc[...] = jnp.zeros_like(dxacc)
    a1[...] = jnp.zeros_like(a1)
    a3[...] = jnp.zeros_like(a3)
    a2[...] = jnp.zeros_like(a2)
    for c in own_loads:
        c.wait()
    og[...] = jnp.transpose(tg[1].astype(F32))

    def t_source(k):
        near_j, near_c = _group(k - 2, 1)
        mid_j, mid_c = _group(k - 8, 4)
        j = jnp.where(k < 2, 0, jnp.where(k < 8, near_j, jnp.where(k < 14, mid_j, 7)))
        c = jnp.where(k < 2, k, jnp.where(k < 8, near_c, jnp.where(k < 14, mid_c, k - 14)))
        return _source(me, j, c)

    def w_source(k):
        q = k - 4
        g = q // 6
        i = q % 6
        gj = jnp.where(g < 2, 1 + i % 3, jnp.where(i < 2, 4, 5 + i % 2))
        gc = jnp.where(g < 2, i // 3, jnp.where(i < 2, i, i // 2 - 1))
        j = jnp.where(k < 4, 0, jnp.where(k < 28, gj, 7))
        c = jnp.where(k < 4, k // 2, jnp.where(k < 28, gc, k % 2))
        slot = jnp.where(k < 4, k % 2, jnp.where(k < 28, g % 2, (k - 28) // 2))
        return _source(me, j, c) * el + slot

    def t_load(k, own):
        b = k % 2
        dev = t_source(k)
        return [pltpu.make_async_copy(x_ref if own else xa.at[dev], tx.at[b], tl_sem.at[b, 0]),
                pltpu.make_async_copy(dy_ref if own else dya.at[dev], tdy.at[b], tl_sem.at[b, 1]),
                pltpu.make_async_copy(gt_ref if own else gta.at[dev], tg.at[b], tl_sem.at[b, 2])]

    def w_load(k, own):
        b = k % 2
        e = w_source(k)
        s = k % 2
        return [pltpu.make_async_copy(w1_ref.at[s] if own else wa1.at[e], v1.at[b], wl_sem.at[b, 0]),
                pltpu.make_async_copy(w3_ref.at[s] if own else wa3.at[e], v3.at[b], wl_sem.at[b, 1]),
                pltpu.make_async_copy(w2_ref.at[s] if own else wa2.at[e], v2.at[b], wl_sem.at[b, 2])]

    def fetch(load, k, owned):
        @pl.when(k < owned)
        def _():
            start(load(k, True))

        @pl.when(k >= owned)
        def _():
            start(load(k, False))

    def any_of(k, values):
        hit = k == values[0]
        for v in values[1:]:
            hit = jnp.logical_or(hit, k == v)
        return hit

    def turn(load, k, owned, starts, count):
        @pl.when(any_of(k, starts))
        def _():
            fetch(load, k, owned)

        @pl.when(jnp.logical_and(k + 1 < count, jnp.logical_not(any_of(k + 1, starts))))
        def _():
            fetch(load, k + 1, owned)

        for c in load(k, False):
            c.wait()

    @pl.loop(0, STEPS)
    def _(s):
        for key, (at, sends) in SERVICE.items():
            @pl.when(s == at)
            def _(key=key, sends=sends):
                for c in received(*key):
                    c.wait_recv()
                start(passed(*key))
                for k in sends:
                    start(sent(*k))

        @pl.when(s == 1)
        def _():
            for c in own_pass_t(other):
                c.wait_recv()

        @pl.when(s == 3)
        def _():
            for c in own_pass_w(other):
                c.wait_recv()

        for at, keys in PASSED.items():
            @pl.when(s == at)
            def _(keys=keys):
                for key in keys:
                    for c in passed_here(*key):
                        c.wait_recv()

        tokens = jnp.logical_or(s < 2, jnp.logical_and(s >= 6, s < 20))

        @pl.when(tokens)
        def _():
            k = jnp.where(s < 2, s, s - 4)
            b = k % 2
            turn(t_load, k, 1, TSTART, 16)

            @pl.loop(0, el)
            def _(e):
                x = tx[b]
                act, do, du, dv = _inner(x, tdy[b], _column(jnp.transpose(tg[b].astype(F32)), me * el + e), o1[e], o3[e], o2[e])
                a1[e] += _dot_tn(x, du)
                a3[e] += _dot_tn(x, dv)
                a2[e] += _dot_tn(act, do)

        @pl.when(jnp.logical_not(tokens))
        def _():
            k = jnp.where(s < 6, s - 2, s - 16)
            b = k % 2
            turn(w_load, k, 2, WSTART, 32)
            g = _column(og[...], w_source(k))
            act, _, du, dv = _inner(ox[...], ody[...], g, v1[b], v3[b], v2[b])
            on = g > 0.0
            o = _dot(act, v2[b]).astype(BF).astype(F32)
            yacc[...] += jnp.where(on, g * o, 0.0)
            dxk = (_dot_nt(du, v1[b]) + _dot_nt(dv, v3[b])).astype(BF).astype(F32)
            dxacc[...] += jnp.where(on, dxk, 0.0)

        @pl.when(s == 20)
        def _():
            for i, (a, d) in enumerate(((a1, d1_ref), (a3, d3_ref), (a2, d2_ref))):
                pltpu.make_async_copy(a, d, out_sem.at[i]).start()

    tx[0] = yacc[...].astype(BF)
    tx[1] = dxacc[...].astype(BF)
    outs = [pltpu.make_async_copy(tx.at[0], y_ref, out_sem.at[3]), pltpu.make_async_copy(tx.at[1], dx_ref, out_sem.at[4])]
    start(outs)
    for i, (a, d) in enumerate(((a1, d1_ref), (a3, d3_ref), (a2, d2_ref))):
        pltpu.make_async_copy(a, d, out_sem.at[i]).wait()
    for key in SERVICE:
        for c in sent(*key) + passed(*key):
            c.wait_send()
    for c in own_pass_t(me) + own_pass_w(me):
        c.wait_send()
    for c in outs:
        c.wait()


def solution(mesh):
    n = mesh.shape['ep']

    def body(xl, rl, gl, dyl, w1l, w3l, w2l):
        tl, d = xl.shape
        el, _, ff = w1l.shape
        nexp = el * n
        hit = rl.T[None] == jnp.arange(nexp)[:, None, None]
        gt = jnp.sum(jnp.where(hit, gl.T.astype(F32)[None], 0.0), axis=1).astype(BF)

        third = -(-tl // 48) * 16
        thirds = ((0, third), (third, (tl - third) // 2), ((tl + third) // 2, (tl - third) // 2))
        dma = pltpu.SemaphoreType.DMA
        out = lambda *s: jax.ShapeDtypeStruct(s, F32)
        outb = lambda *s: jax.ShapeDtypeStruct(s, BF)
        nw = len(WROUNDS)
        hbm = pl.BlockSpec(memory_space=pl.ANY)
        res = pl.pallas_call(
            functools.partial(_kernel, el, thirds),
            out_shape=[outb(tl, d), outb(tl, d), out(el, d, ff), out(el, d, ff), out(el, ff, d),
                       outb(n, tl, d), outb(n, tl, d), outb(n, nexp, tl), outb(nexp, d, ff), outb(nexp, d, ff), outb(nexp, ff, d)],
            in_specs=[hbm] * 6,
            out_specs=[hbm] * 11,
            scratch_shapes=[
                pltpu.VMEM((2, tl, d), BF), pltpu.VMEM((2, tl, d), BF), pltpu.VMEM((2, nexp, tl), BF),
                pltpu.VMEM((2, d, ff), BF), pltpu.VMEM((2, d, ff), BF), pltpu.VMEM((2, ff, d), BF),
                pltpu.VMEM((el, d, ff), BF), pltpu.VMEM((el, d, ff), BF), pltpu.VMEM((el, ff, d), BF),
                pltpu.VMEM((tl, d), BF), pltpu.VMEM((tl, d), BF), pltpu.VMEM((tl, nexp), F32),
                pltpu.VMEM((tl, d), F32), pltpu.VMEM((tl, d), F32),
                pltpu.VMEM((el, d, ff), F32), pltpu.VMEM((el, d, ff), F32), pltpu.VMEM((el, ff, d), F32),
                dma((7, 3, 3)), dma((7, 3, 3)), dma((nw, 3)), dma((nw, 3)),
                dma((7, 3, 3)), dma((7, 3, 3)), dma((nw, 3)), dma((nw, 3)),
                dma((3,)), dma((3,)), dma((el, 3)), dma((el, 3)),
                dma((2, 3)), dma((2, 3)), dma((6,)), dma((5,)),
            ],
            compiler_params=pltpu.CompilerParams(collective_id=0, has_side_effects=True, vmem_limit_bytes=67043328),
            name='moe',
        )(xl, dyl, gt, w1l, w3l, w2l)
        return tuple(res[:5])

    spec_t = P('ep', None)
    spec_w = P('ep', None, None)
    return jax.shard_map(body, mesh=mesh, in_specs=(spec_t, spec_t, spec_t, spec_t, spec_w, spec_w, spec_w), out_specs=(spec_t, spec_t, spec_w, spec_w, spec_w), check_vma=False)
```

```python
import functools

import jax
import jax.numpy as jnp
from jax import lax
from jax.experimental import pallas as pl
from jax.experimental.pallas import tpu as pltpu
from jax.sharding import PartitionSpec as P

F32 = jnp.float32
BF = jnp.bfloat16
MESH = pl.DeviceIdType.MESH
NT = (((1,), (1,)), ((), ()))
TN = (((0,), (0,)), ((), ()))
BITS = (2, 4, 8)

ROUNDS = (
    lambda l: (l, ()),
    lambda l: ((l + 2) % 3, ()),
    lambda l: ((l + 1) % 3, ()),
    lambda l: ((l + 2) % 3, ((l + 2) % 3,)),
    lambda l: ((l + 1) % 3, ((l + 1) % 3,)),
    lambda l: ((l + 1) % 3, ((l + 2) % 3,)),
    lambda l: ((l + 1) % 3, ((l + 1) % 3, (l + 2) % 3)),
)
SPREAD = ((4, 3, 5), (3, 5, 4), (4, 3, 5))
WROUNDS = ([(0, r) for r in range(3)] + [(1, r) for r in range(3)] + [(0, r) for r in range(3, 6)]
           + [(1, r) for r in range(3, 6)] + [(0, 6), (1, 6)])
SERVICE = {
    ('t', 0): (3, [('t', 3), ('t', 4)]),
    ('t', 1): (6, [('t', 5)]),
    ('t', 2): (6, []),
    ('t', 3): (9, [('t', 6), ('w', 0)]),
    ('t', 4): (11, [('w', 1)]),
    ('t', 5): (12, [('w', 2)]),
    ('t', 6): (15, [('w', 3)]),
    ('w', 0): (16, [('w', 4)]),
    ('w', 1): (18, [('w', 5)]),
    ('w', 2): (19, [('w', 6)]),
    ('w', 3): (22, [('w', 7)]),
    ('w', 4): (24, [('w', 8)]),
    ('w', 5): (26, [('w', 9)]),
    ('w', 6): (30, [('w', 10)]),
    ('w', 7): (32, [('w', 11)]),
    ('w', 8): (34, [('w', 12)]),
    ('w', 9): (38, []),
    ('w', 10): (38, [('w', 13)]),
    ('w', 11): (40, []),
    ('w', 12): (44, []),
}
LAST = ('w', 13)
PASSED = {8: [('t', r) for r in range(3)], 14: [('t', r) for r in range(3, 6)], 18: [('t', 6)],
          22: [('w', r) for r in range(3)], 28: [('w', r) for r in range(3, 6)], 33: [('w', 6), ('w', 7)], 35: [('w', 8)],
          39: [('w', 9), ('w', 10)], 41: [('w', 11)], 45: [('w', 12)]}
TSTART = (0, 1, 2, 8)
WSTART = (0, 4, 10, 16, 17, 18, 22, 23, 24, 28, 29)
STEPS = 46


def _dot(a, b):
    return jnp.dot(a, b, preferred_element_type=F32)


def _dot_nt(a, b):
    return lax.dot_general(a, b, NT, preferred_element_type=F32)


def _dot_tn(a, b):
    return lax.dot_general(a, b, TN, preferred_element_type=F32)


def _column(gd, e):
    lane = lax.broadcasted_iota(jnp.int32, gd.shape, 1)
    return jnp.sum(jnp.where(lane == e, gd, 0.0), axis=1, keepdims=True)


def _inner(x, dy, g, w1, w3, w2):
    on = g > 0.0
    u = _dot(x, w1)
    v = _dot(x, w3)
    sig = jax.nn.sigmoid(u)
    su = u * sig
    do = (g * dy.astype(F32)).astype(BF)
    da = _dot_nt(do, w2)
    act = jnp.where(on, su * v, 0.0).astype(BF)
    du = jnp.where(on, da * v * (sig * (1.0 + u * (1.0 - sig))), 0.0).astype(BF)
    dv = jnp.where(on, da * su, 0.0).astype(BF)
    return act, do, du, dv


def _expert(x, dy, g, w1, w3, w2):
    act, _, du, dv = _inner(x, dy, g, w1, w3, w2)
    on = g > 0.0
    o = _dot(act, w2).astype(BF).astype(F32)
    dxk = (_dot_nt(du, w1) + _dot_nt(dv, w3)).astype(BF).astype(F32)
    return jnp.where(on, g * o, 0.0), jnp.where(on, dxk, 0.0)


def _flip(dev, bit):
    return dev + bit * (1 - 2 * ((dev // bit) % 2))


def _cross(dev, links):
    for l in links:
        dev = _flip(dev, BITS[l])
    return dev


def _source(me, j, c):
    m = j + jnp.where(j == 3, 1, 0) - jnp.where(j == 4, 1, 0)
    dev = me
    for i, on in enumerate((c, m % 2, (m // 2) % 2, m // 4)):
        bit = 2 ** i
        dev = dev + on * bit * (1 - 2 * ((me // bit) % 2))
    return dev


def _group(q, base):
    return base + q % 3, q // 3


def _kernel(el, thirds, x_ref, dy_ref, gt_ref, w1_ref, w3_ref, w2_ref,
            yf_ref, dxf_ref, d1_ref, d3_ref, d2_ref, xa, dya, gta, wa1, wa3, wa2,
            tx, tdy, tg, v1, v3, v2, o1, o3, o2, ox, ody, og, yacc, dxacc, a1, a3, a2,
            ts, tr, ws, wr, tps, tpr, wps, wpr, tos, tor, wos, wor, tl_sem, wl_sem, own_sem, out_sem):
    me = lax.axis_index('ep')
    other = _flip(me, 1)
    near = [_flip(me, b) for b in BITS]

    def remote(src, dst, ssem, rsem, dev):
        return pltpu.make_async_remote_copy(src_ref=src, dst_ref=dst, send_sem=ssem, recv_sem=rsem,
                                            device_id=(dev,), device_id_type=MESH)

    def pieces(kind, r, p, dev, mine, k):
        if kind == 't':
            rows = pl.ds(*thirds[p])
            gate = [(gt_ref if mine else gta.at[dev], gta.at[dev], (r, k, 2))] if p == 1 else []
            return gate + [((x_ref if mine else xa.at[dev]).at[rows], xa.at[dev, rows], (r, k, 0)),
                           ((dy_ref if mine else dya.at[dev]).at[rows], dya.at[dev, rows], (r, k, 1))]
        slot = WROUNDS[r][0]
        own, far = ((w1_ref, wa1), (w3_ref, wa3), (w2_ref, wa2))[p]
        return [(own.at[slot] if mine else far.at[dev * el + slot], far.at[dev * el + slot], (r, k))]

    def leg(kind, r, l):
        i = r if kind == 't' else WROUNDS[r][1]
        if kind == 'w' and 3 <= i < 6:
            i = SPREAD[l][i - 3]
        return ROUNDS[i](l)

    def sent(kind, r):
        ss, rs = (ts, tr) if kind == 't' else (ws, wr)
        out = []
        for l in range(3):
            p, path = leg(kind, r, l)
            for src, dst, i in pieces(kind, r, p, _cross(me, path), not path, l):
                out.append(remote(src, dst, ss.at[i], rs.at[i], near[l]))
        return out

    def arrived(kind, r, at, ss, rs, dev):
        out = []
        for l in range(3):
            p, path = leg(kind, r, l)
            for _, dst, i in pieces(kind, r, p, _cross(at, path + (l,)), False, l):
                out.append(remote(dst, dst, ss.at[i], rs.at[i], near[l] if dev is None else dev))
        return out

    def received(kind, r):
        return arrived(kind, r, me, *((ts, tr) if kind == 't' else (ws, wr)), None)

    def passed(kind, r):
        return arrived(kind, r, me, *((tps, tpr) if kind == 't' else (wps, wpr)), other)

    def passed_here(kind, r):
        return arrived(kind, r, other, *((tps, tpr) if kind == 't' else (wps, wpr)), other)

    def own_pass_t(dev):
        return [remote(x_ref, xa.at[dev], tos.at[0], tor.at[0], other),
                remote(dy_ref, dya.at[dev], tos.at[1], tor.at[1], other),
                remote(gt_ref, gta.at[dev], tos.at[2], tor.at[2], other)]

    def own_pass_w(dev):
        return [remote(own.at[s], far.at[dev * el + s], wos.at[s, i], wor.at[s, i], other)
                for s in range(el) for i, (own, far) in enumerate(((w1_ref, wa1), (w3_ref, wa3), (w2_ref, wa2)))]

    def start(copies):
        for c in copies:
            c.start()

    own_loads = [pltpu.make_async_copy(a, b, own_sem.at[i]) for i, (a, b) in enumerate((
        (x_ref, ox), (dy_ref, ody), (gt_ref, tg.at[1]), (w1_ref, o1), (w3_ref, o3), (w2_ref, o2)))]
    start(own_loads)

    barrier = pltpu.get_barrier_semaphore()
    for dev in near + [other]:
        pl.semaphore_signal(barrier, inc=1, device_id=(dev,), device_id_type=MESH)
    pl.semaphore_wait(barrier, 4)
    for r in range(3):
        start(sent('t', r))
    start(own_pass_t(me))
    start(own_pass_w(me))

    yacc[...] = jnp.zeros_like(yacc)
    dxacc[...] = jnp.zeros_like(dxacc)
    a1[...] = jnp.zeros_like(a1)
    a3[...] = jnp.zeros_like(a3)
    a2[...] = jnp.zeros_like(a2)
    for c in own_loads:
        c.wait()
    og[...] = jnp.transpose(tg[1].astype(F32))

    def t_source(k):
        near_j, near_c = _group(k - 2, 1)
        mid_j, mid_c = _group(k - 8, 4)
        j = jnp.where(k < 2, 0, jnp.where(k < 8, near_j, jnp.where(k < 14, mid_j, 7)))
        c = jnp.where(k < 2, k, jnp.where(k < 8, near_c, jnp.where(k < 14, mid_c, k - 14)))
        return _source(me, j, c)

    def w_source(k):
        q = k - 4
        g = q // 6
        i = q % 6
        gj = jnp.where(g < 2, 1 + i % 3, jnp.where(i < 2, 4, 5 + i % 2))
        gc = jnp.where(g < 2, i // 3, jnp.where(i < 2, i, i // 2 - 1))
        j = jnp.where(k < 4, 0, jnp.where(k < 28, gj, 7))
        c = jnp.where(k < 4, k // 2, jnp.where(k < 28, gc, k % 2))
        slot = jnp.where(k < 4, k % 2, jnp.where(k < 28, g % 2, (k - 28) // 2))
        return _source(me, j, c) * el + slot

    def t_load(k, own):
        b = k % 2
        dev = t_source(k)
        return [pltpu.make_async_copy(x_ref if own else xa.at[dev], tx.at[b], tl_sem.at[b, 0]),
                pltpu.make_async_copy(dy_ref if own else dya.at[dev], tdy.at[b], tl_sem.at[b, 1]),
                pltpu.make_async_copy(gt_ref if own else gta.at[dev], tg.at[b], tl_sem.at[b, 2])]

    def w_load(k, own):
        b = k % 2
        e = w_source(k)
        s = k % 2
        return [pltpu.make_async_copy(w1_ref.at[s] if own else wa1.at[e], v1.at[b], wl_sem.at[b, 0]),
                pltpu.make_async_copy(w3_ref.at[s] if own else wa3.at[e], v3.at[b], wl_sem.at[b, 1]),
                pltpu.make_async_copy(w2_ref.at[s] if own else wa2.at[e], v2.at[b], wl_sem.at[b, 2])]

    def fetch(load, k, owned):
        @pl.when(k < owned)
        def _():
            start(load(k, True))

        @pl.when(k >= owned)
        def _():
            start(load(k, False))

    def any_of(k, values):
        hit = k == values[0]
        for v in values[1:]:
            hit = jnp.logical_or(hit, k == v)
        return hit

    def turn(load, k, owned, starts, count):
        @pl.when(any_of(k, starts))
        def _():
            fetch(load, k, owned)

        @pl.when(jnp.logical_and(k + 1 < count, jnp.logical_not(any_of(k + 1, starts))))
        def _():
            fetch(load, k + 1, owned)

        for c in load(k, False):
            c.wait()

    @pl.loop(0, STEPS)
    def _(s):
        for key, (at, sends) in SERVICE.items():
            @pl.when(s == at)
            def _(key=key, sends=sends):
                for c in received(*key):
                    c.wait_recv()
                start(passed(*key))
                for k in sends:
                    start(sent(*k))

        @pl.when(s == 1)
        def _():
            for c in own_pass_t(other):
                c.wait_recv()

        @pl.when(s == 3)
        def _():
            for c in own_pass_w(other):
                c.wait_recv()

        for at, keys in PASSED.items():
            @pl.when(s == at)
            def _(keys=keys):
                for key in keys:
                    for c in passed_here(*key):
                        c.wait_recv()

        tokens = jnp.logical_or(s < 2, jnp.logical_and(s >= 6, s < 20))

        @pl.when(tokens)
        def _():
            k = jnp.where(s < 2, s, s - 4)
            b = k % 2
            turn(t_load, k, 1, TSTART, 16)

            @pl.loop(0, el)
            def _(e):
                x = tx[b]
                act, do, du, dv = _inner(x, tdy[b], _column(jnp.transpose(tg[b].astype(F32)), me * el + e), o1[e], o3[e], o2[e])
                a1[e] += _dot_tn(x, du)
                a3[e] += _dot_tn(x, dv)
                a2[e] += _dot_tn(act, do)

        @pl.when(jnp.logical_not(tokens))
        def _():
            k = jnp.where(s < 6, s - 2, s - 16)
            b = k % 2
            turn(w_load, k, 2, WSTART, 30)
            yk, dxk = _expert(ox[...], ody[...], _column(og[...], w_source(k)), v1[b], v3[b], v2[b])
            yacc[...] += yk
            dxacc[...] += dxk

        @pl.when(s == 20)
        def _():
            for i, (a, d) in enumerate(((a1, d1_ref), (a3, d3_ref), (a2, d2_ref))):
                pltpu.make_async_copy(a, d, out_sem.at[i]).start()

    outs = [pltpu.make_async_copy(yacc, yf_ref, out_sem.at[3]), pltpu.make_async_copy(dxacc, dxf_ref, out_sem.at[4])]
    start(outs)
    for c in received(*LAST):
        c.wait_recv()
    start(passed(*LAST))
    for i, (a, d) in enumerate(((a1, d1_ref), (a3, d3_ref), (a2, d2_ref))):
        pltpu.make_async_copy(a, d, out_sem.at[i]).wait()
    for key in list(SERVICE) + [LAST]:
        for c in sent(*key):
            c.wait_send()
    for key in SERVICE:
        for c in passed(*key):
            c.wait_send()
    for c in own_pass_t(me) + own_pass_w(me):
        c.wait_send()
    for c in outs:
        c.wait()
    for c in passed_here(*LAST):
        c.wait_recv()
    for c in passed(*LAST):
        c.wait_send()


def _finish_kernel(el, x_ref, dy_ref, gt_ref, wa1, wa3, wa2, yf_ref, dxf_ref, e1_ref, e3_ref, e2_ref,
                   y_ref, dx_ref, d1_ref, d3_ref, d2_ref,
                   ox, ody, tg, v1, v3, v2, yacc, dxacc, yo, dxo, a1, a3, a2, in_sem, w_sem, acc_sem, d_sem, o_sem):
    me = lax.axis_index('ep')
    far = _cross(me, (0, 1, 2))
    experts = [far * el + el - 1, _flip(far, 1) * el + el - 1]
    copy = pltpu.make_async_copy

    def begin(pairs, sem):
        copies = [copy(a, b, sem.at[i]) for i, (a, b) in enumerate(pairs)]
        for c in copies:
            c.start()
        return copies

    def finish(copies):
        for c in copies:
            c.wait()

    def weights(i):
        e = experts[i]
        return begin(((wa1.at[e], v1.at[i]), (wa3.at[e], v3.at[i]), (wa2.at[e], v2.at[i])), w_sem.at[i])

    tokens = begin(((gt_ref, tg), (x_ref, ox), (dy_ref, ody)), in_sem)
    first = weights(0)
    finish(tokens)
    finish(first)
    acc = begin(((yf_ref, yacc), (dxf_ref, dxacc)), acc_sem)
    second = weights(1)
    grads = begin(((e1_ref, a1), (e3_ref, a3), (e2_ref, a2)), d_sem)
    gd = jnp.transpose(tg[...].astype(F32))
    yk, dxk = _expert(ox[...], ody[...], _column(gd, experts[0]), v1[0], v3[0], v2[0])
    finish(acc)
    yacc[...] += yk
    dxacc[...] += dxk
    finish(second)
    finish(grads)
    outs = begin(((a1, d1_ref), (a3, d3_ref), (a2, d2_ref)), o_sem)
    yk, dxk = _expert(ox[...], ody[...], _column(gd, experts[1]), v1[1], v3[1], v2[1])
    yo[...] = (yacc[...] + yk).astype(BF)
    dxo[...] = (dxacc[...] + dxk).astype(BF)
    last = begin(((yo, y_ref), (dxo, dx_ref)), in_sem)
    finish(outs)
    finish(last)


def solution(mesh):
    n = mesh.shape['ep']

    def body(xl, rl, gl, dyl, w1l, w3l, w2l):
        tl, d = xl.shape
        el, _, ff = w1l.shape
        nexp = el * n
        hit = rl.T[None] == jnp.arange(nexp)[:, None, None]
        gt = jnp.sum(jnp.where(hit, gl.T.astype(F32)[None], 0.0), axis=1).astype(BF)

        mid = tl // 48 * 16
        thirds = ((0, (tl - mid) // 2), ((tl - mid) // 2, mid), ((tl + mid) // 2, (tl - mid) // 2))
        dma = pltpu.SemaphoreType.DMA
        out = lambda *s: jax.ShapeDtypeStruct(s, F32)
        outb = lambda *s: jax.ShapeDtypeStruct(s, BF)
        nw = len(WROUNDS)
        hbm = pl.BlockSpec(memory_space=pl.ANY)
        res = pl.pallas_call(
            functools.partial(_kernel, el, thirds),
            out_shape=[out(tl, d), out(tl, d), out(el, d, ff), out(el, d, ff), out(el, ff, d),
                       outb(n, tl, d), outb(n, tl, d), outb(n, nexp, tl), outb(nexp, d, ff), outb(nexp, d, ff), outb(nexp, ff, d)],
            in_specs=[hbm] * 6,
            out_specs=[hbm] * 11,
            scratch_shapes=[
                pltpu.VMEM((2, tl, d), BF), pltpu.VMEM((2, tl, d), BF), pltpu.VMEM((2, nexp, tl), BF),
                pltpu.VMEM((2, d, ff), BF), pltpu.VMEM((2, d, ff), BF), pltpu.VMEM((2, ff, d), BF),
                pltpu.VMEM((el, d, ff), BF), pltpu.VMEM((el, d, ff), BF), pltpu.VMEM((el, ff, d), BF),
                pltpu.VMEM((tl, d), BF), pltpu.VMEM((tl, d), BF), pltpu.VMEM((tl, nexp), F32),
                pltpu.VMEM((tl, d), F32), pltpu.VMEM((tl, d), F32),
                pltpu.VMEM((el, d, ff), F32), pltpu.VMEM((el, d, ff), F32), pltpu.VMEM((el, ff, d), F32),
                dma((7, 3, 3)), dma((7, 3, 3)), dma((nw, 3)), dma((nw, 3)),
                dma((7, 3, 3)), dma((7, 3, 3)), dma((nw, 3)), dma((nw, 3)),
                dma((3,)), dma((3,)), dma((el, 3)), dma((el, 3)),
                dma((2, 3)), dma((2, 3)), dma((6,)), dma((5,)),
            ],
            compiler_params=pltpu.CompilerParams(collective_id=0, has_side_effects=True, vmem_limit_bytes=67043328),
            name='moe',
        )(xl, dyl, gt, w1l, w3l, w2l)
        wa1, wa3, wa2 = res[8:]
        return tuple(pl.pallas_call(
            functools.partial(_finish_kernel, el),
            out_shape=[outb(tl, d), outb(tl, d), out(el, d, ff), out(el, d, ff), out(el, ff, d)],
            in_specs=[hbm] * 11,
            out_specs=[hbm] * 5,
            scratch_shapes=[
                pltpu.VMEM((tl, d), BF), pltpu.VMEM((tl, d), BF), pltpu.VMEM((nexp, tl), BF),
                pltpu.VMEM((2, d, ff), BF), pltpu.VMEM((2, d, ff), BF), pltpu.VMEM((2, ff, d), BF),
                pltpu.VMEM((tl, d), F32), pltpu.VMEM((tl, d), F32), pltpu.VMEM((tl, d), BF), pltpu.VMEM((tl, d), BF),
                pltpu.VMEM((el, d, ff), F32), pltpu.VMEM((el, d, ff), F32), pltpu.VMEM((el, ff, d), F32),
                dma((3,)), dma((2, 3)), dma((2,)), dma((3,)), dma((3,)),
            ],
            compiler_params=pltpu.CompilerParams(vmem_limit_bytes=67043328),
            name='finish',
        )(xl, dyl, gt, wa1, wa3, wa2, *res[:5]))

    spec_t = P('ep', None)
    spec_w = P('ep', None, None)
    return jax.shard_map(body, mesh=mesh, in_specs=(spec_t, spec_t, spec_t, spec_t, spec_w, spec_w, spec_w), out_specs=(spec_t, spec_t, spec_w, spec_w, spec_w), check_vma=False)
```
